32 devices in a mesh: batch: 4 (over x, core), rows: 8 (over z, y).
Axes of the slice: x: 2, y: 2, z: 4, core: 2. Of those that a mesh axis runs over, the one named last changes fastest.
Arguments:
- feat_quarter: bfloat16 [4, 128, 512, 256], P('batch', 'rows'), may hold values from -12 to 12
- feat_eighth: bfloat16 [4, 64, 256, 256], P('batch', 'rows'), may hold values from -12 to 12
- feat_sixteenth: bfloat16 [4, 32, 128, 256], P('batch', 'rows'), may hold values from -12 to 12
- feat_thirty: bfloat16 [4, 16, 64, 256], P('batch', 'rows'), may hold values from -12 to 12
- labels: int32 [4, 128, 512], P('batch', 'rows'), may hold values from 0 to 255, as said below
- first_weights: bfloat16 [4, 3, 3, 256, 128], replicated, may hold values from -0.125 to 0.125
- inner_weights: bfloat16 [3, 3, 3, 128, 128], replicated, may hold values from -0.1875 to 0.1875
- norm_gain: float32 [7, 128], replicated, may hold values from 0.1 to 1.9
- norm_shift: float32 [7, 128], replicated, may hold values from -3 to 3
- class_weight: bfloat16 [128, 19], replicated, may hold values from -0.5 to 0.5
- class_bias: float32 [19], replicated, may hold values from -3 to 3
Outputs:
- logits: bfloat16 [4, 19, 128, 512], P('batch', None, 'rows')
- mean_loss: float32 [], replicated
The draws below stay inside these ranges and needn't reach their ends.
Inputs may be any that keep to these rules, and one draw needn't show every extreme that they name: `labels`: values 0 to 18 name classes; 255 marks a pixel without a label.
All inputs are finite; a program needn't handle non-finite values.
Results may differ from the reference program's by a relative error of at most 0.008.
Values may be sent and summed in bfloat16 or wider, within the bound.
A program may use at most 128 MiB of HBM per device.

```python
import jax
import jax.numpy as jnp
from jax import lax

C_IN = 256
HEAD = 128
CLASSES = 19
GROUPS = 32
COLS4 = 512
IMAGES = 4
QUARTER_ROWS = 128


def feature_map(key, row_count, col_count, marker):
    level_key = jax.random.fold_in(key, marker)
    base_key, offset_key, slope_key = jax.random.split(level_key, 3)
    array_shape = (IMAGES, row_count, col_count, C_IN)
    row_ramp = ((jnp.arange(row_count, dtype=jnp.float32) + 0.5) / row_count)[None, :, None, None]
    base = jax.random.normal(base_key, array_shape, jnp.float32)
    slope_rate = jax.random.uniform(slope_key, (IMAGES, 1, 1, 1), jnp.float32, 1.0, 1.6)
    offset = jax.random.normal(offset_key, (IMAGES, 1, 1, C_IN), jnp.float32) * 0.5
    row_scale = jnp.exp(1.4 * slope_rate * (row_ramp - 0.5))
    values = base * row_scale + 2.0 * offset * row_ramp
    return jnp.clip(values, -12.0, 12.0).astype(jnp.bfloat16)


def draw_feat_quarter(key, part):
    return feature_map(key, QUARTER_ROWS, COLS4, 11)


def draw_feat_eighth(key, part):
    return feature_map(key, QUARTER_ROWS // 2, COLS4 // 2, 12)


def draw_feat_sixteenth(key, part):
    return feature_map(key, QUARTER_ROWS // 4, COLS4 // 4, 13)


def draw_feat_thirty(key, part):
    return feature_map(key, QUARTER_ROWS // 8, COLS4 // 8, 14)


def draw_labels(key, part):
    class_key, drop_key, major_key, choose_key = jax.random.split(jax.random.fold_in(key, 7), 4)
    array_shape = (IMAGES, QUARTER_ROWS, COLS4)
    classes = jax.random.randint(class_key, array_shape, 0, CLASSES)
    majors = jax.random.randint(major_key, (IMAGES, QUARTER_ROWS // 8), 0, CLASSES)
    row_index = jnp.arange(QUARTER_ROWS, dtype=jnp.int32)
    block_major = majors[:, row_index // 8][:, :, None]
    choose = jax.random.randint(choose_key, array_shape, 0, 1000)
    classes = jnp.where(choose < 700, block_major, classes)
    chance = jax.random.randint(drop_key, array_shape, 0, 1000)
    drop_limit = 40 + 700 * row_index * row_index // (QUARTER_ROWS * QUARTER_ROWS)
    return jnp.where(chance < drop_limit[None, :, None], 255, classes).astype(jnp.int32)


def centred(key, dims, scale, bound, held_as=jnp.bfloat16):
    drawn = jax.random.normal(key, dims, jnp.float32) * scale
    return jnp.minimum(jnp.maximum(drawn, -bound), bound).astype(held_as)


def setup_inputs(seed: int = 0) -> dict:
    arg_keys = jax.random.split(jax.random.key(seed), 12)
    feat_quarter = draw_feat_quarter(jax.random.fold_in(arg_keys[11], 71), 0)
    feat_eighth = draw_feat_eighth(jax.random.fold_in(arg_keys[11], 71), 0)
    feat_sixteenth = draw_feat_sixteenth(jax.random.fold_in(arg_keys[11], 71), 0)
    feat_thirty = draw_feat_thirty(jax.random.fold_in(arg_keys[11], 71), 0)
    labels = draw_labels(jax.random.fold_in(arg_keys[11], 71), 0)
    first_weights = centred(arg_keys[5], (4, 3, 3, C_IN, HEAD), (9 * C_IN) ** -0.5, 0.125)
    inner_weights = centred(arg_keys[6], (3, 3, 3, HEAD, HEAD), (9 * HEAD) ** -0.5, 0.1875)
    norm_gain = jnp.clip(1.0 + 0.18 * jax.random.normal(arg_keys[7], (7, HEAD), jnp.float32), 0.1, 1.9)
    norm_shift = centred(arg_keys[8], (7, HEAD), 0.5, 3.0, jnp.float32)
    class_weight = centred(arg_keys[9], (HEAD, CLASSES), HEAD ** -0.5, 0.5)
    class_bias = centred(arg_keys[10], (CLASSES,), 0.5, 3.0, jnp.float32)
    return {"feat_quarter": feat_quarter, "feat_eighth": feat_eighth, "feat_sixteenth": feat_sixteenth, "feat_thirty": feat_thirty, "labels": labels, "first_weights": first_weights, "inner_weights": inner_weights, "norm_gain": norm_gain, "norm_shift": norm_shift, "class_weight": class_weight, "class_bias": class_bias}


NORM_FLOOR = 0.05

def conv_rows(framed, weight):
    row_count = framed.shape[0] - 2
    col_count = framed.shape[1]
    padded = jnp.pad(framed, ((0, 0), (1, 1), (0, 0)))
    result = jnp.zeros((row_count, col_count, weight.shape[3]), jnp.float32)
    for downward in range(3):
        for across in range(3):
            window = padded[downward:downward + row_count, across:across + col_count, :]
            result = result + jnp.einsum('rwc,cd->rwd', window.astype(jnp.float32), weight[downward, across].astype(jnp.float32))
    return result

def heighten(padded):
    row_count = padded.shape[0] - 2
    middle = padded[1:-1]
    even_rows = 0.75 * middle + 0.25 * padded[:-2]
    odd_rows = 0.75 * middle + 0.25 * padded[2:]
    inner_rows = jnp.stack([even_rows, odd_rows], axis=1).reshape(2 * row_count, padded.shape[1], padded.shape[2])
    upper_row = 0.75 * padded[0] + 0.25 * padded[1]
    lower_row = 0.75 * padded[-1] + 0.25 * padded[-2]
    return jnp.concatenate([upper_row[None], inner_rows, lower_row[None]], axis=0)

def widen(field):
    left_side = jnp.concatenate([field[:, :1], field[:, :-1]], axis=1)
    right_side = jnp.concatenate([field[:, 1:], field[:, -1:]], axis=1)
    even_cols = 0.75 * field + 0.25 * left_side
    odd_cols = 0.75 * field + 0.25 * right_side
    return jnp.stack([even_cols, odd_cols], axis=2).reshape(field.shape[0], 2 * field.shape[1], field.shape[2])

def group_sum(values):
    channel_sums = lax.optimization_barrier(jnp.sum(values, axis=(0, 1)))
    return channel_sums.reshape(GROUPS, -1).sum(axis=1)

def spread(values, width):
    return jnp.repeat(values, width // GROUPS)

def finish(values, group_mean, group_var, gain, shift):
    width = values.shape[2]
    factor = gain * lax.rsqrt(spread(group_var, width) + NORM_FLOOR)
    return jnp.maximum((values - spread(group_mean, width)) * factor + shift, 0.0).astype(jnp.bfloat16)

def normalize(values, gain, shift):
    pixels = values.shape[0] * values.shape[1] * (values.shape[2] // GROUPS)
    group_mean = group_sum(values) / pixels
    centered = values - spread(group_mean, values.shape[2])
    group_var = group_sum(centered * centered) / pixels
    return finish(values, group_mean, group_var, gain, shift)

def upsample(active):
    padded = jnp.pad(active, ((1, 1), (0, 0), (0, 0)), mode='edge').astype(jnp.float32)
    return widen(heighten(padded)[1:-1]).astype(jnp.bfloat16)

def reference(feat_quarter, feat_eighth, feat_sixteenth, feat_thirty, labels, first_weights, inner_weights, norm_gain, norm_shift, class_weight, class_bias):

    def section(image_in, weight, layer_index):
        framed = jnp.pad(image_in, ((1, 1), (0, 0), (0, 0)))
        return normalize(conv_rows(framed, weight), norm_gain[layer_index], norm_shift[layer_index])

    def one_image(image_items):
        quarter_in, eighth_in, sixteenth_in, thirty_in, label_map = image_items
        quarter = section(quarter_in, first_weights[0], 0)
        eighth = upsample(section(eighth_in, first_weights[1], 1))
        sixteenth = upsample(section(upsample(section(sixteenth_in, first_weights[2], 2)), inner_weights[0], 4))
        coarse = upsample(section(thirty_in, first_weights[3], 3))
        thirty = upsample(section(upsample(section(coarse, inner_weights[1], 5)), inner_weights[2], 6))
        combined = (quarter.astype(jnp.float32) + eighth.astype(jnp.float32) + sixteenth.astype(jnp.float32) + thirty.astype(jnp.float32)).astype(jnp.bfloat16)
        scores = jnp.einsum('rwc,ck->krw', combined.astype(jnp.float32), class_weight.astype(jnp.float32)) + class_bias.astype(jnp.float32)[:, None, None]
        log_total = jnp.log(lax.optimization_barrier(jnp.sum(jnp.exp(scores), axis=0)))
        classes = jnp.arange(scores.shape[0], dtype=jnp.int32)[:, None, None]
        picked = lax.optimization_barrier(jnp.sum(jnp.where(classes == label_map[None], scores, 0.0), axis=0))
        usable = label_map != 255
        loss_total = jnp.sum(jnp.where(usable, log_total - picked, 0.0))
        valid_count = jnp.sum(usable.astype(jnp.float32))
        return (scores.astype(jnp.bfloat16), loss_total, valid_count)
    logits, totals, counts = lax.map(one_image, (feat_quarter, feat_eighth, feat_sixteenth, feat_thirty, labels))
    mean_loss = jnp.sum(totals) / jnp.maximum(jnp.sum(counts), 1.0)
    return (logits, mean_loss)
```

```python
import functools

import jax
import jax.numpy as jnp
from jax import lax
from jax.experimental import pallas as pl
from jax.experimental.pallas import tpu as pltpu
from jax.sharding import PartitionSpec as P

GROUPS = 32
NORM_FLOOR = 0.05
MESH = pl.DeviceIdType.MESH


def exchange_kernel(shape, axes, x_ref, out_ref, send_sem, recv_sem):
    coords = [lax.axis_index(axis) for axis in shape]
    names = list(shape)
    total = 1
    for axis in axes:
        total *= shape[axis]

    def peer(distance):
        ids = list(coords)
        rest = distance
        for axis in reversed(axes):
            size = shape[axis]
            ids[names.index(axis)] = lax.rem(coords[names.index(axis)] + rest % size, size)
            rest //= size
        return tuple(ids)

    barrier = pltpu.get_barrier_semaphore()
    for d in range(1, total):
        pl.semaphore_signal(barrier, inc=1, device_id=peer(d), device_id_type=MESH)
    pl.semaphore_wait(barrier, total - 1)
    copies = []
    for d in range(1, total):
        copy = pltpu.make_async_remote_copy(
            src_ref=x_ref,
            dst_ref=out_ref.at[d],
            send_sem=send_sem.at[d],
            recv_sem=recv_sem.at[d],
            device_id=peer(d),
            device_id_type=MESH,
        )
        copy.start()
        copies.append(copy)
    out_ref[0] = x_ref[...]
    for copy in copies:
        copy.wait()


def exchange(x, shape, axes, collective_id):
    total = 1
    for axis in axes:
        total *= shape[axis]
    return pl.pallas_call(
        functools.partial(exchange_kernel, shape, axes),
        out_shape=jax.ShapeDtypeStruct((total,) + x.shape, x.dtype),
        in_specs=[pl.BlockSpec(memory_space=pltpu.VMEM)],
        out_specs=pl.BlockSpec(memory_space=pltpu.VMEM),
        scratch_shapes=[pltpu.SemaphoreType.DMA((total,)), pltpu.SemaphoreType.DMA((total,))],
        compiler_params=pltpu.CompilerParams(collective_id=collective_id, has_side_effects=True),
    )(x)


def conv(framed, weight):
    return lax.conv_general_dilated(
        framed[None],
        weight,
        (1, 1),
        ((0, 0), (1, 1)),
        dimension_numbers=("NHWC", "HWIO", "NHWC"),
        preferred_element_type=jnp.float32,
    )[0]


def halo_rows(array, width):
    size, length = lax.axis_size("rows"), array.shape[0]
    before, after = [], []
    step = 1
    while width > 0:
        take = min(width, length)
        up = [(i, i + step) for i in range(size - step)]
        down = [(j, i) for i, j in up]
        before.insert(0, lax.ppermute(array[length - take :], "rows", up))
        after.append(lax.ppermute(array[:take], "rows", down))
        width -= take
        step += 1
    return before, after


def framed_by(array, width):
    before, after = halo_rows(array, width)
    return jnp.concatenate(before + [array] + after, axis=0)


def fold(values):
    return values.reshape(GROUPS, -1).sum(axis=1)


def spread(values, width):
    return jnp.repeat(values, width // GROUPS)


def double_rows(field, axis):
    count = field.shape[axis]
    first = lax.slice_in_dim(field, 0, count - 1, axis=axis)
    second = lax.slice_in_dim(field, 1, count, axis=axis)
    lines = jnp.stack([0.75 * first + 0.25 * second, 0.25 * first + 0.75 * second], axis=axis + 1)
    return lines.reshape(field.shape[:axis] + (2 * count - 2,) + field.shape[axis + 1 :])


def col_matrix(cols):
    source = lax.broadcasted_iota(jnp.int32, (cols, 2 * cols), 0)
    target = lax.broadcasted_iota(jnp.int32, (cols, 2 * cols), 1)
    near = target // 2
    far = jnp.clip(near + 2 * (target % 2) - 1, 0, cols - 1)
    return 0.75 * (source == near) + 0.25 * (source == far)


def make_per_device(shape):
    def per_device(
        feat_quarter,
        feat_eighth,
        feat_sixteenth,
        feat_thirty,
        labels,
        first_weights,
        inner_weights,
        norm_gain,
        norm_shift,
        class_weight,
        class_bias,
    ):
        position = lax.axis_index("rows")
        size = shape["rows"]

        def statistics(fields, call):
            slab, counts = [], []
            width = fields[0].shape[2]
            for y in fields:
                count = y.shape[0] * y.shape[1] * (width // GROUPS)
                sums = y.sum(axis=(0, 1))
                mean = spread(fold(sums) / count, width)
                square = (y - mean) ** 2
                slab += [sums, square.sum(axis=(0, 1))]
                counts.append(count)
            slab += [jnp.zeros_like(slab[0])] * (-len(slab) % 8)
            all_slabs = exchange(jnp.stack(slab), shape, ("rows",), call)
            folded = all_slabs.reshape(size, -1, GROUPS, width // GROUPS).sum(axis=3)
            result = []
            for i, count in enumerate(counts):
                means = folded[:, 2 * i] / count
                mean = means.mean(axis=0)
                spread_squares = count * ((means - mean) ** 2).sum(axis=0)
                var = (folded[:, 2 * i + 1].sum(axis=0) + spread_squares) / (count * size)
                result.append((mean, var))
            return result

        def activate(y, stat, layer):
            width = y.shape[2]
            factor = norm_gain[layer] * lax.rsqrt(spread(stat[1], width) + NORM_FLOOR)
            return jnp.maximum(
                (y - spread(stat[0], width)) * factor + norm_shift[layer], 0.0
            ).astype(jnp.bfloat16)

        def rows_of(count, own, extra):
            return position * own + lax.broadcasted_iota(jnp.int32, (count, 1, 1), 0) - extra

        def double(act, own, extra, kept):
            numbers = rows_of(act.shape[0], own, extra)
            top, bottom = act[extra : extra + 1], act[extra + own - 1 : extra + own]
            act = jnp.where(numbers < 0, top, jnp.where(numbers >= own * size, bottom, act))
            wide = jnp.einsum(
                "rwc,wv->rvc",
                act,
                col_matrix(act.shape[1]).astype(jnp.bfloat16),
                preferred_element_type=jnp.float32,
            )
            cut = 2 * extra - 1 - kept
            grown = double_rows(wide, 0)[cut : cut + 2 * own + 2 * kept].astype(jnp.bfloat16)
            lines = rows_of(grown.shape[0], 2 * own, kept)
            inside = (lines >= 0) & (lines < 2 * own * size)
            return jnp.where(inside, grown, jnp.zeros_like(grown))

        q, e, s, t = feat_quarter[0], feat_eighth[0], feat_sixteenth[0], feat_thirty[0]
        t_own, s_own, e_own = t.shape[0], s.shape[0], e.shape[0]
        t_framed = framed_by(t, 3)
        s_framed = framed_by(s, 2)
        e_framed = framed_by(e, 1)
        q_framed = framed_by(q, 1)
        t_out = conv(t_framed, first_weights[3])
        s_out = conv(s_framed, first_weights[2])
        t_stat, s_stat = statistics([t_out[2:-2], s_out[1:-1]], 0)
        t_out = conv(double(activate(t_out, t_stat, 3), t_own, 2, 2), inner_weights[1])
        s_out = conv(double(activate(s_out, s_stat, 2), s_own, 1, 1), inner_weights[0])
        e_out = conv(e_framed, first_weights[1])
        t_stat, s_stat, e_stat = statistics([t_out[1:-1], s_out, e_out], 1)
        s_act = activate(s_out, s_stat, 4)
        e_act = activate(e_out, e_stat, 1)
        t_out = conv(double(activate(t_out, t_stat, 5), 2 * t_own, 1, 1), inner_weights[2])
        q_out = conv(q_framed, first_weights[0])
        t_stat, q_stat = statistics([t_out, q_out], 2)
        t_act = activate(t_out, t_stat, 6)
        q_act = activate(q_out, q_stat, 0)

        coarse = jnp.einsum(
            "rwc,ck->krw",
            jnp.concatenate([e_act, s_act, t_act], axis=2),
            jnp.concatenate([class_weight] * 3, axis=0),
            preferred_element_type=jnp.float32,
        )
        up = [(i, i + 1) for i in range(size - 1)]
        down = [(j, i) for i, j in up]
        before = lax.ppermute(coarse[:, -1:], "rows", up)
        after = lax.ppermute(coarse[:, :1], "rows", down)
        before = jnp.where(position == 0, coarse[:, :1], before)
        after = jnp.where(position == size - 1, coarse[:, -1:], after)
        coarse = jnp.concatenate([before, coarse, after], axis=1)
        wide = jnp.einsum(
            "krw,wv->krv",
            coarse,
            col_matrix(coarse.shape[2]),
            precision=lax.Precision.HIGHEST,
            preferred_element_type=jnp.float32,
        )
        grown = double_rows(wide, 1)[:, 1:-1]
        scores = (
            jnp.einsum("rwc,ck->krw", q_act, class_weight, preferred_element_type=jnp.float32)
            + grown
            + class_bias[:, None, None]
        )
        log_total = jnp.log(jnp.sum(jnp.exp(scores), axis=0))
        label_map = labels[0]
        classes = jnp.arange(scores.shape[0], dtype=jnp.int32)[:, None, None]
        picked = jnp.sum(jnp.where(classes == label_map[None], scores, 0.0), axis=0)
        usable = label_map != 255
        local_total = jnp.sum(jnp.where(usable, log_total - picked, 0.0))
        local_count = jnp.sum(usable.astype(jnp.float32))
        lane = lax.broadcasted_iota(jnp.int32, (8, 128), 1)
        slab = jnp.where(lane == 0, local_total, jnp.where(lane == 1, local_count, 0.0))
        sums = exchange(slab, shape, ("batch", "rows"), 3)[:, 0].sum(axis=0)
        mean_loss = sums[0] / jnp.maximum(sums[1], 1.0)
        return (scores.astype(jnp.bfloat16)[None], mean_loss)

    return per_device


def solution(mesh):
    in_specs = (
        P("batch", "rows", None, None),
        P("batch", "rows", None, None),
        P("batch", "rows", None, None),
        P("batch", "rows", None, None),
        P("batch", "rows", None),
        P(),
        P(),
        P(),
        P(),
        P(),
        P(),
    )
    out_specs = (P("batch", None, "rows", None), P())
    return jax.shard_map(
        make_per_device(dict(mesh.shape)),
        mesh=mesh,
        in_specs=in_specs,
        out_specs=out_specs,
        check_vma=False,
    )
```

```python
import functools

import jax
import jax.numpy as jnp
from jax import lax
from jax.experimental import pallas as pl
from jax.experimental.pallas import tpu as pltpu
from jax.sharding import PartitionSpec as P

GROUPS = 32
NORM_FLOOR = 0.05
MESH = pl.DeviceIdType.MESH


def exchange_kernel(shape, axes, x_ref, out_ref, send_sem, recv_sem):
    coords = [lax.axis_index(axis) for axis in shape]
    names = list(shape)
    total = 1
    for axis in axes:
        total *= shape[axis]

    def peer(distance):
        ids = list(coords)
        rest = distance
        for axis in reversed(axes):
            size = shape[axis]
            ids[names.index(axis)] = lax.rem(coords[names.index(axis)] + rest % size, size)
            rest //= size
        return tuple(ids)

    barrier = pltpu.get_barrier_semaphore()
    for d in range(1, total):
        pl.semaphore_signal(barrier, inc=1, device_id=peer(d), device_id_type=MESH)
    pl.semaphore_wait(barrier, total - 1)
    copies = []
    for d in range(1, total):
        copy = pltpu.make_async_remote_copy(
            src_ref=x_ref,
            dst_ref=out_ref.at[d],
            send_sem=send_sem.at[d],
            recv_sem=recv_sem.at[d],
            device_id=peer(d),
            device_id_type=MESH,
        )
        copy.start()
        copies.append(copy)
    out_ref[0] = x_ref[...]
    for copy in copies:
        copy.wait()


def exchange(x, shape, axes, collective_id):
    total = 1
    for axis in axes:
        total *= shape[axis]
    return pl.pallas_call(
        functools.partial(exchange_kernel, shape, axes),
        out_shape=jax.ShapeDtypeStruct((total,) + x.shape, x.dtype),
        in_specs=[pl.BlockSpec(memory_space=pltpu.VMEM)],
        out_specs=pl.BlockSpec(memory_space=pltpu.VMEM),
        scratch_shapes=[pltpu.SemaphoreType.DMA((total,)), pltpu.SemaphoreType.DMA((total,))],
        compiler_params=pltpu.CompilerParams(collective_id=collective_id, has_side_effects=True),
    )(x)


def conv_kernel(rows, x_ref, w_ref, y_ref, stat_ref, flat_ref):
    cols, depth = x_ref.shape[1:]
    width = w_ref.shape[3]
    step = pl.program_id(0)

    @pl.when(step == 0)
    def _():
        for down in range(3):
            for across in range(3):
                flat_ref[
                    down * depth : (down + 1) * depth, across * width : (across + 1) * width
                ] = w_ref[down, across]

    lhs = jnp.concatenate(
        [
            x_ref[pl.ds(step * rows + down, rows)].reshape(rows * cols, depth)
            for down in range(3)
        ],
        axis=1,
    )
    taps = jnp.dot(lhs, flat_ref[...], preferred_element_type=jnp.float32)
    col = lax.rem(lax.broadcasted_iota(jnp.int32, (rows * cols, width), 0), cols)
    left = jnp.where(col == 0, 0.0, pltpu.roll(taps[:, :width], 1, 0))
    right = jnp.where(col == cols - 1, 0.0, pltpu.roll(taps[:, 2 * width :], rows * cols - 1, 0))
    y = (taps[:, width : 2 * width] + left + right).reshape(rows, cols, width)
    y_ref[...] = y
    sums = jnp.sum(y, axis=1, keepdims=True)
    centred = y - sums / cols
    stat_ref[:, 0:1] = sums
    stat_ref[:, 1:2] = jnp.sum(centred * centred, axis=1, keepdims=True)


def conv(framed, weight):
    count, cols, depth = framed.shape
    count -= 2
    width = weight.shape[3]
    rows = max(r for r in range(1, count + 1) if count % r == 0 and (r == 1 or r * cols <= 1024))
    return pl.pallas_call(
        functools.partial(conv_kernel, rows),
        grid=(count // rows,),
        out_shape=(
            jax.ShapeDtypeStruct((count, cols, width), jnp.float32),
            jax.ShapeDtypeStruct((count, 2, width), jnp.float32),
        ),
        in_specs=[
            pl.BlockSpec(framed.shape, lambda i: (0, 0, 0)),
            pl.BlockSpec(weight.shape, lambda i: (0, 0, 0, 0)),
        ],
        out_specs=(
            pl.BlockSpec((rows, cols, width), lambda i: (i, 0, 0)),
            pl.BlockSpec((rows, 2, width), lambda i: (i, 0, 0)),
        ),
        scratch_shapes=[pltpu.VMEM((3 * depth, 3 * width), jnp.bfloat16)],
        cost_estimate=pl.CostEstimate(
            flops=18 * count * cols * depth * width,
            bytes_accessed=2 * framed.size + 4 * count * cols * width,
            transcendentals=0,
        ),
    )(framed, weight)


def framed_by(arrays, widths):
    size = lax.axis_size("rows")
    lengths = [array.shape[0] for array in arrays]
    before, after = ([[] for _ in arrays] for _ in range(2))
    step = 1
    left = list(widths)
    while any(left):
        takes = [min(w, n) for w, n in zip(left, lengths)]
        up = [(i, i + step) for i in range(size - step)]
        down = [(j, i) for i, j in up]
        for pairs, side, last in ((up, before, True), (down, after, False)):
            parts = [
                (a[n - k :] if last else a[:k]).reshape(-1, a.shape[2])
                for a, n, k in zip(arrays, lengths, takes)
                if k
            ]
            packed = parts[0] if len(parts) == 1 else jnp.concatenate(parts, axis=0)
            got = lax.ppermute(packed, "rows", pairs)
            start = 0
            for index, (a, k) in enumerate(zip(arrays, takes)):
                if k:
                    end = start + k * a.shape[1]
                    piece = got[start:end].reshape((k,) + a.shape[1:])
                    side[index].insert(0 if last else len(side[index]), piece)
                    start = end
        left = [w - k for w, k in zip(left, takes)]
        step += 1
    return [
        jnp.concatenate(x + [a] + z, axis=0) for x, a, z in zip(before, arrays, after)
    ]


def fold(values):
    return values.reshape(GROUPS, -1).sum(axis=1)


def spread(values, width):
    return jnp.repeat(values, width // GROUPS)


def double_rows(field, axis):
    count = field.shape[axis]
    first = lax.slice_in_dim(field, 0, count - 1, axis=axis)
    second = lax.slice_in_dim(field, 1, count, axis=axis)
    lines = jnp.stack([0.75 * first + 0.25 * second, 0.25 * first + 0.75 * second], axis=axis + 1)
    return lines.reshape(field.shape[:axis] + (2 * count - 2,) + field.shape[axis + 1 :])


def col_matrix(cols):
    source = lax.broadcasted_iota(jnp.int32, (cols, 2 * cols), 0)
    target = lax.broadcasted_iota(jnp.int32, (cols, 2 * cols), 1)
    near = target // 2
    far = jnp.clip(near + 2 * (target % 2) - 1, 0, cols - 1)
    return 0.75 * (source == near) + 0.25 * (source == far)


def make_per_device(shape):
    def per_device(
        feat_quarter,
        feat_eighth,
        feat_sixteenth,
        feat_thirty,
        labels,
        first_weights,
        inner_weights,
        norm_gain,
        norm_shift,
        class_weight,
        class_bias,
    ):
        position = lax.axis_index("rows")
        size = shape["rows"]

        def statistics(fields):
            slab, counts = [], []
            for rows, cols in fields:
                width = rows.shape[2]
                count = rows.shape[0] * cols * (width // GROUPS)
                sums = rows[:, 0].sum(axis=0)
                mean = spread(fold(sums) / count, width)
                strays = cols * ((rows[:, 0] / cols - mean) ** 2).sum(axis=0)
                slab += [sums, rows[:, 1].sum(axis=0) + strays]
                counts.append(count)
            slab += [jnp.zeros_like(slab[0])] * (-len(slab) % 8)
            all_slabs = exchange(jnp.stack(slab), shape, ("rows",), 0)
            folded = all_slabs.reshape(size, -1, GROUPS, width // GROUPS).sum(axis=3)
            result = []
            for i, count in enumerate(counts):
                means = folded[:, 2 * i] / count
                mean = means.mean(axis=0)
                spread_squares = count * ((means - mean) ** 2).sum(axis=0)
                var = (folded[:, 2 * i + 1].sum(axis=0) + spread_squares) / (count * size)
                result.append((mean, var))
            return result

        def activate(y, stat, layer):
            width = y.shape[2]
            factor = norm_gain[layer] * lax.rsqrt(spread(stat[1], width) + NORM_FLOOR)
            return jnp.maximum(
                (y - spread(stat[0], width)) * factor + norm_shift[layer], 0.0
            ).astype(jnp.bfloat16)

        def rows_of(count, own, extra):
            return position * own + lax.broadcasted_iota(jnp.int32, (count, 1, 1), 0) - extra

        def double(act, own, extra, kept):
            numbers = rows_of(act.shape[0], own, extra)
            top, bottom = act[extra : extra + 1], act[extra + own - 1 : extra + own]
            act = jnp.where(numbers < 0, top, jnp.where(numbers >= own * size, bottom, act))
            wide = jnp.einsum(
                "rwc,wv->rvc",
                act,
                col_matrix(act.shape[1]).astype(jnp.bfloat16),
                preferred_element_type=jnp.float32,
            )
            cut = 2 * extra - 1 - kept
            grown = double_rows(wide, 0)[cut : cut + 2 * own + 2 * kept].astype(jnp.bfloat16)
            lines = rows_of(grown.shape[0], 2 * own, kept)
            inside = (lines >= 0) & (lines < 2 * own * size)
            return jnp.where(inside, grown, jnp.zeros_like(grown))

        q, e, s, t = feat_quarter[0], feat_eighth[0], feat_sixteenth[0], feat_thirty[0]
        t_own, s_own, e_own = t.shape[0], s.shape[0], e.shape[0]
        t_framed, s_framed = framed_by([t, s], [3, 2])
        e_framed, q_framed = framed_by([e, q], [1, 1])
        t_out, t_sum = conv(t_framed, first_weights[3])
        s_out, s_sum = conv(s_framed, first_weights[2])
        t_stat, s_stat = statistics([(t_sum[2:-2], t_out.shape[1]), (s_sum[1:-1], s_out.shape[1])])
        t_out, t_sum = conv(double(activate(t_out, t_stat, 3), t_own, 2, 2), inner_weights[1])
        s_out, s_sum = conv(double(activate(s_out, s_stat, 2), s_own, 1, 1), inner_weights[0])
        e_out, e_sum = conv(e_framed, first_weights[1])
        t_stat, s_stat, e_stat = statistics(
            [(t_sum[1:-1], t_out.shape[1]), (s_sum, s_out.shape[1]), (e_sum, e_out.shape[1])]
        )
        s_act = activate(s_out, s_stat, 4)
        e_act = activate(e_out, e_stat, 1)
        t_out, t_sum = conv(double(activate(t_out, t_stat, 5), 2 * t_own, 1, 1), inner_weights[2])
        q_out, q_sum = conv(q_framed, first_weights[0])
        t_stat, q_stat = statistics([(t_sum, t_out.shape[1]), (q_sum, q_out.shape[1])])
        t_act = activate(t_out, t_stat, 6)
        q_act = activate(q_out, q_stat, 0)

        coarse = jnp.einsum(
            "rwc,ck->krw",
            jnp.concatenate([e_act, s_act, t_act], axis=2),
            jnp.concatenate([class_weight] * 3, axis=0),
            preferred_element_type=jnp.float32,
        )
        up = [(i, i + 1) for i in range(size - 1)]
        down = [(j, i) for i, j in up]
        before = lax.ppermute(coarse[:, -1:], "rows", up)
        after = lax.ppermute(coarse[:, :1], "rows", down)
        before = jnp.where(position == 0, coarse[:, :1], before)
        after = jnp.where(position == size - 1, coarse[:, -1:], after)
        coarse = jnp.concatenate([before, coarse, after], axis=1)
        wide = jnp.einsum(
            "krw,wv->krv",
            coarse,
            col_matrix(coarse.shape[2]),
            precision=lax.Precision.HIGHEST,
            preferred_element_type=jnp.float32,
        )
        grown = double_rows(wide, 1)[:, 1:-1]
        scores = (
            jnp.einsum("rwc,ck->krw", q_act, class_weight, preferred_element_type=jnp.float32)
            + grown
            + class_bias[:, None, None]
        )
        log_total = jnp.log(jnp.sum(jnp.exp(scores), axis=0))
        label_map = labels[0]
        classes = jnp.arange(scores.shape[0], dtype=jnp.int32)[:, None, None]
        picked = jnp.sum(jnp.where(classes == label_map[None], scores, 0.0), axis=0)
        usable = label_map != 255
        local_total = jnp.sum(jnp.where(usable, log_total - picked, 0.0))
        local_count = jnp.sum(usable.astype(jnp.float32))
        lane = lax.broadcasted_iota(jnp.int32, (8, 128), 1)
        slab = jnp.where(lane == 0, local_total, jnp.where(lane == 1, local_count, 0.0))
        sums = exchange(slab, shape, ("rows",), 0).sum(axis=0)
        sums = exchange(sums, shape, ("batch",), 1)[:, 0].sum(axis=0)
        mean_loss = sums[0] / jnp.maximum(sums[1], 1.0)
        return (scores.astype(jnp.bfloat16)[None], mean_loss)

    return per_device


def solution(mesh):
    in_specs = (
        P("batch", "rows", None, None),
        P("batch", "rows", None, None),
        P("batch", "rows", None, None),
        P("batch", "rows", None, None),
        P("batch", "rows", None),
        P(),
        P(),
        P(),
        P(),
        P(),
        P(),
    )
    out_specs = (P("batch", None, "rows", None), P())
    return jax.shard_map(
        make_per_device(dict(mesh.shape)),
        mesh=mesh,
        in_specs=in_specs,
        out_specs=out_specs,
        check_vma=False,
    )
```

```python
import functools

import jax
import jax.numpy as jnp
import numpy as np
from jax import lax
from jax.experimental import pallas as pl
from jax.experimental.pallas import tpu as pltpu
from jax.sharding import PartitionSpec as P

GROUPS = 32
NORM_FLOOR = 0.05
MESH = pl.DeviceIdType.MESH


def exchange_kernel(shape, axes, x_ref, out_ref, send_sem, recv_sem):
    coords = [lax.axis_index(axis) for axis in shape]
    names = list(shape)
    total = 1
    for axis in axes:
        total *= shape[axis]

    def peer(distance):
        ids = list(coords)
        rest = distance
        for axis in reversed(axes):
            size = shape[axis]
            ids[names.index(axis)] = lax.rem(coords[names.index(axis)] + rest % size, size)
            rest //= size
        return tuple(ids)

    barrier = pltpu.get_barrier_semaphore()
    for d in range(1, total):
        pl.semaphore_signal(barrier, inc=1, device_id=peer(d), device_id_type=MESH)
    pl.semaphore_wait(barrier, total - 1)
    copies = []
    for d in range(1, total):
        copy = pltpu.make_async_remote_copy(
            src_ref=x_ref,
            dst_ref=out_ref.at[d],
            send_sem=send_sem.at[d],
            recv_sem=recv_sem.at[d],
            device_id=peer(d),
            device_id_type=MESH,
        )
        copy.start()
        copies.append(copy)
    out_ref[0] = x_ref[...]
    for copy in copies:
        copy.wait()


def exchange(x, shape, axes, collective_id):
    total = 1
    for axis in axes:
        total *= shape[axis]
    return pl.pallas_call(
        functools.partial(exchange_kernel, shape, axes),
        out_shape=jax.ShapeDtypeStruct((total,) + x.shape, x.dtype),
        in_specs=[pl.BlockSpec(memory_space=pltpu.VMEM)],
        out_specs=pl.BlockSpec(memory_space=pltpu.VMEM),
        scratch_shapes=[pltpu.SemaphoreType.DMA((total,)), pltpu.SemaphoreType.DMA((total,))],
        compiler_params=pltpu.CompilerParams(collective_id=collective_id, has_side_effects=True),
    )(x)


def conv_kernel(rows, x_ref, w_ref, y_ref, stat_ref, flat_ref):
    cols, depth = x_ref.shape[1:]
    width = w_ref.shape[3]
    step = pl.program_id(0)

    @pl.when(step == 0)
    def _():
        for down in range(3):
            for across in range(3):
                flat_ref[
                    down * depth : (down + 1) * depth, across * width : (across + 1) * width
                ] = w_ref[down, across]

    lhs = jnp.concatenate(
        [
            x_ref[pl.ds(step * rows + down, rows)].reshape(rows * cols, depth)
            for down in range(3)
        ],
        axis=1,
    )
    taps = jnp.dot(lhs, flat_ref[...], preferred_element_type=jnp.float32)
    col = lax.rem(lax.broadcasted_iota(jnp.int32, (rows * cols, width), 0), cols)
    left = jnp.where(col == 0, 0.0, pltpu.roll(taps[:, :width], 1, 0))
    right = jnp.where(col == cols - 1, 0.0, pltpu.roll(taps[:, 2 * width :], rows * cols - 1, 0))
    y = (taps[:, width : 2 * width] + left + right).reshape(rows, cols, width)
    y_ref[...] = y
    sums = jnp.sum(y, axis=1, keepdims=True)
    centred = y - sums / cols
    stat_ref[:, 0:1] = sums
    stat_ref[:, 1:2] = jnp.sum(centred * centred, axis=1, keepdims=True)


def conv(framed, weight):
    count, cols, depth = framed.shape
    count -= 2
    width = weight.shape[3]
    rows = max(r for r in range(1, count + 1) if count % r == 0 and (r == 1 or r * cols <= 1024))
    return pl.pallas_call(
        functools.partial(conv_kernel, rows),
        grid=(count // rows,),
        out_shape=(
            jax.ShapeDtypeStruct((count, cols, width), jnp.float32),
            jax.ShapeDtypeStruct((count, 2, width), jnp.float32),
        ),
        in_specs=[
            pl.BlockSpec(framed.shape, lambda i: (0, 0, 0)),
            pl.BlockSpec(weight.shape, lambda i: (0, 0, 0, 0)),
        ],
        out_specs=(
            pl.BlockSpec((rows, cols, width), lambda i: (i, 0, 0)),
            pl.BlockSpec((rows, 2, width), lambda i: (i, 0, 0)),
        ),
        scratch_shapes=[pltpu.VMEM((3 * depth, 3 * width), jnp.bfloat16)],
        cost_estimate=pl.CostEstimate(
            flops=18 * count * cols * depth * width,
            bytes_accessed=2 * framed.size + 4 * count * cols * width,
            transcendentals=0,
        ),
    )(framed, weight)


def edges_kernel(size, widths, *refs):
    many = len(widths)
    arrays, before, after = refs[:many], refs[many : 2 * many], refs[2 * many : 3 * many]
    send_sem, recv_sem = refs[3 * many :]
    me = lax.axis_index("rows")
    reach = max(-(-w // a.shape[0]) for a, w in zip(arrays, widths))
    barrier = pltpu.get_barrier_semaphore()
    sides = [side * step for step in range(1, reach + 1) for side in (1, -1)]

    def exists(offset):
        return me + offset < size if offset > 0 else me + offset >= 0

    def target(offset):
        return {"rows": lax.rem(me + offset + size, size)}

    for offset in sides:

        @pl.when(exists(offset))
        def _():
            pl.semaphore_signal(
                barrier, inc=1, device_id=target(offset), device_id_type=MESH
            )

    peers = jnp.minimum(me, reach) + jnp.minimum(size - 1 - me, reach)
    pl.semaphore_wait(barrier, peers)

    copies = []
    for index in reversed(range(many)):
        array, width = arrays[index], widths[index]
        length = array.shape[0]
        done, step = 0, 1
        while done < width:
            take = min(width - done, length)
            for offset in (step, -step):
                if offset > 0:
                    source = array.at[length - take : length]
                    landing = before[index].at[width - done - take : width - done]
                else:
                    source = array.at[0:take]
                    landing = after[index].at[done : done + take]
                copy = pltpu.make_async_remote_copy(
                    src_ref=source,
                    dst_ref=landing,
                    send_sem=send_sem.at[len(copies)],
                    recv_sem=recv_sem.at[len(copies)],
                    device_id=target(offset),
                    device_id_type=MESH,
                )
                copies.append((copy, offset, landing))
                pl.when(exists(offset))(copy.start)
            done += take
            step += 1
    for copy, offset, landing in copies:

        @pl.when(jnp.logical_not(exists(-offset)))
        def _():
            landing[...] = jnp.zeros(landing.shape, landing.dtype)

        pl.when(exists(offset))(copy.wait_send)
        pl.when(exists(-offset))(copy.wait_recv)


def edges(arrays, widths, size, collective_id):
    outs = [jax.ShapeDtypeStruct((w,) + a.shape[1:], a.dtype) for a, w in zip(arrays, widths)]
    copies = 2 * sum(-(-w // a.shape[0]) for a, w in zip(arrays, widths))
    got = pl.pallas_call(
        functools.partial(edges_kernel, size, tuple(widths)),
        out_shape=tuple(outs + outs),
        in_specs=[pl.BlockSpec(memory_space=pl.ANY)] * len(arrays),
        out_specs=tuple([pl.BlockSpec(memory_space=pltpu.VMEM)] * (2 * len(arrays))),
        scratch_shapes=[pltpu.SemaphoreType.DMA((copies,)), pltpu.SemaphoreType.DMA((copies,))],
        compiler_params=pltpu.CompilerParams(collective_id=collective_id, has_side_effects=True),
    )(*arrays)
    return got[: len(arrays)], got[len(arrays) :]


def fold(values):
    return values.reshape(GROUPS, -1).sum(axis=1)


def spread(values, width):
    return jnp.repeat(values, width // GROUPS)


def double_rows(field, axis):
    count = field.shape[axis]
    first = lax.slice_in_dim(field, 0, count - 1, axis=axis)
    second = lax.slice_in_dim(field, 1, count, axis=axis)
    lines = jnp.stack([0.75 * first + 0.25 * second, 0.25 * first + 0.75 * second], axis=axis + 1)
    return lines.reshape(field.shape[:axis] + (2 * count - 2,) + field.shape[axis + 1 :])


def col_matrix(cols):
    target = np.arange(2 * cols)
    near = target // 2
    far = np.clip(near + 2 * (target % 2) - 1, 0, cols - 1)
    source = np.arange(cols)[:, None]
    return (0.75 * (source == near) + 0.25 * (source == far)).astype(np.float32)


def make_per_device(shape):
    def per_device(
        feat_quarter,
        feat_eighth,
        feat_sixteenth,
        feat_thirty,
        labels,
        first_weights,
        inner_weights,
        norm_gain,
        norm_shift,
        class_weight,
        class_bias,
    ):
        position = lax.axis_index("rows")
        size = shape["rows"]

        def statistics(fields):
            slab, counts = [], []
            for rows, cols in fields:
                width = rows.shape[2]
                count = rows.shape[0] * cols * (width // GROUPS)
                sums = rows[:, 0].sum(axis=0)
                mean = spread(fold(sums) / count, width)
                strays = cols * ((rows[:, 0] / cols - mean) ** 2).sum(axis=0)
                slab += [sums, rows[:, 1].sum(axis=0) + strays]
                counts.append(count)
            slab += [jnp.zeros_like(slab[0])] * (-len(slab) % 8)
            all_slabs = exchange(jnp.stack(slab), shape, ("rows",), 0)
            folded = all_slabs.reshape(size, -1, GROUPS, width // GROUPS).sum(axis=3)
            result = []
            for i, count in enumerate(counts):
                means = folded[:, 2 * i] / count
                mean = means.mean(axis=0)
                spread_squares = count * ((means - mean) ** 2).sum(axis=0)
                var = (folded[:, 2 * i + 1].sum(axis=0) + spread_squares) / (count * size)
                result.append((mean, var))
            return result

        def activate(y, stat, layer):
            width = y.shape[2]
            factor = norm_gain[layer] * lax.rsqrt(spread(stat[1], width) + NORM_FLOOR)
            return jnp.maximum(
                (y - spread(stat[0], width)) * factor + norm_shift[layer], 0.0
            ).astype(jnp.bfloat16)

        def rows_of(dims, own, extra):
            return position * own + lax.broadcasted_iota(jnp.int32, dims, 0) - extra

        def double(act, own, extra, kept):
            numbers = rows_of(act.shape, own, extra)
            top, bottom = act[extra : extra + 1], act[extra + own - 1 : extra + own]
            act = jnp.where(numbers < 0, top, jnp.where(numbers >= own * size, bottom, act))
            wide = jnp.einsum(
                "rwc,wv->rvc",
                act,
                jnp.asarray(col_matrix(act.shape[1]), jnp.bfloat16),
                preferred_element_type=jnp.float32,
            )
            cut = 2 * extra - 1 - kept
            grown = double_rows(wide, 0)[cut : cut + 2 * own + 2 * kept].astype(jnp.bfloat16)
            lines = rows_of(grown.shape, 2 * own, kept)
            inside = (lines >= 0) & (lines < 2 * own * size)
            return jnp.where(inside, grown, jnp.zeros_like(grown))

        q, e, s, t = feat_quarter[0], feat_eighth[0], feat_sixteenth[0], feat_thirty[0]
        t_own, s_own, e_own = t.shape[0], s.shape[0], e.shape[0]
        bands = [q, e, s, t]
        q_framed, e_framed, s_framed, t_framed = [
            jnp.concatenate([x, band, z], axis=0)
            for x, band, z in zip(*((lambda g: (g[0], bands, g[1]))(edges(bands, [1, 1, 2, 3], size, 2))))
        ]
        t_out, t_sum = conv(t_framed, first_weights[3])
        s_out, s_sum = conv(s_framed, first_weights[2])
        t_stat, s_stat = statistics([(t_sum[2:-2], t_out.shape[1]), (s_sum[1:-1], s_out.shape[1])])
        t_out, t_sum = conv(double(activate(t_out, t_stat, 3), t_own, 2, 2), inner_weights[1])
        s_out, s_sum = conv(double(activate(s_out, s_stat, 2), s_own, 1, 1), inner_weights[0])
        e_out, e_sum = conv(e_framed, first_weights[1])
        t_stat, s_stat, e_stat = statistics(
            [(t_sum[1:-1], t_out.shape[1]), (s_sum, s_out.shape[1]), (e_sum, e_out.shape[1])]
        )
        s_act = activate(s_out, s_stat, 4)
        e_act = activate(e_out, e_stat, 1)
        t_out, t_sum = conv(double(activate(t_out, t_stat, 5), 2 * t_own, 1, 1), inner_weights[2])
        q_out, q_sum = conv(q_framed, first_weights[0])
        t_stat, q_stat = statistics([(t_sum, t_out.shape[1]), (q_sum, q_out.shape[1])])
        t_act = activate(t_out, t_stat, 6)
        q_act = activate(q_out, q_stat, 0)

        coarse = jnp.einsum(
            "rwc,ck->rkw",
            jnp.concatenate([e_act, s_act, t_act], axis=2),
            jnp.concatenate([class_weight] * 3, axis=0),
            preferred_element_type=jnp.float32,
        )
        (before,), (after,) = edges([coarse], [1], size, 3)
        before = jnp.where(position == 0, coarse[:1], before)
        after = jnp.where(position == size - 1, coarse[-1:], after)
        coarse = jnp.concatenate([before, coarse, after], axis=0).transpose(1, 0, 2)
        wide = jnp.einsum(
            "krw,wv->krv",
            coarse,
            col_matrix(coarse.shape[2]),
            precision=lax.Precision.HIGHEST,
            preferred_element_type=jnp.float32,
        )
        grown = double_rows(wide, 1)[:, 1:-1]
        scores = (
            jnp.einsum("rwc,ck->krw", q_act, class_weight, preferred_element_type=jnp.float32)
            + grown
            + class_bias[:, None, None]
        )
        log_total = jnp.log(jnp.sum(jnp.exp(scores), axis=0))
        label_map = labels[0]
        classes = jnp.arange(scores.shape[0], dtype=jnp.int32)[:, None, None]
        picked = jnp.sum(jnp.where(classes == label_map[None], scores, 0.0), axis=0)
        usable = label_map != 255
        local_total = jnp.sum(jnp.where(usable, log_total - picked, 0.0))
        local_count = jnp.sum(usable.astype(jnp.float32))
        lane = lax.broadcasted_iota(jnp.int32, (8, 128), 1)
        slab = jnp.where(lane == 0, local_total, jnp.where(lane == 1, local_count, 0.0))
        sums = exchange(slab, shape, ("rows",), 0).sum(axis=0)
        sums = exchange(sums, shape, ("batch",), 1)[:, 0].sum(axis=0)
        mean_loss = sums[0] / jnp.maximum(sums[1], 1.0)
        return (scores.astype(jnp.bfloat16)[None], mean_loss)

    return per_device


def solution(mesh):
    in_specs = (
        P("batch", "rows", None, None),
        P("batch", "rows", None, None),
        P("batch", "rows", None, None),
        P("batch", "rows", None, None),
        P("batch", "rows", None),
        P(),
        P(),
        P(),
        P(),
        P(),
        P(),
    )
    out_specs = (P("batch", None, "rows", None), P())
    return jax.shard_map(
        make_per_device(dict(mesh.shape)),
        mesh=mesh,
        in_specs=in_specs,
        out_specs=out_specs,
        check_vma=False,
    )
```
